16 devices in a mesh: dp: 2 (over z), tp: 8 (over y, x, core).
Axes of the slice: x: 2, y: 2, z: 2, core: 2. Of those that a mesh axis runs over, the one named last changes fastest.
Arguments:
- x_chunk: bfloat16 [16, 1024, 2560], P('dp', 'tp'), parts along dimension 0
- prefix_len: int32 [16], P('dp'), parts along dimension 0
- k_cache: bfloat16 [16, 2048, 32, 80], P('dp', None, 'tp'), parts along dimension 0
- v_cache: bfloat16 [16, 2048, 32, 80], P('dp', None, 'tp'), parts along dimension 0
- ln1_gain: bfloat16 [2560], replicated
- ln1_bias: bfloat16 [2560], replicated
- w_qkv: bfloat16 [2560, 7680], P(None, 'tp')
- b_qkv: bfloat16 [7680], P('tp')
- w_out: bfloat16 [2560, 2560], P('tp')
- b_out: bfloat16 [2560], replicated
- ln2_gain: bfloat16 [2560], replicated
- ln2_bias: bfloat16 [2560], replicated
- w_up: bfloat16 [2560, 10240], P(None, 'tp')
- b_up: bfloat16 [10240], P('tp')
- w_down: bfloat16 [10240, 2560], P('tp')
- b_down: bfloat16 [2560], replicated
Outputs:
- output 1: bfloat16 [16, 1024, 2560], P('dp', 'tp'), parts along dimension 0
- output 2: bfloat16 [16, 2048, 32, 80], P('dp', None, 'tp'), parts along dimension 0
- output 3: bfloat16 [16, 2048, 32, 80], P('dp', None, 'tp'), parts along dimension 0
There are 2 independent parts. The reference program is written for one: setup_inputs(seed, part) draws one part's arguments, and reference() takes and returns one part's arrays. A program takes and returns all parts, laid end to end along the dimension named above; an argument that names none is the same for every part.
All inputs are finite; a program needn't handle non-finite values.
Results may differ from the reference program's by a relative error of at most 0.0126204.
Values are sent between devices in bfloat16 or wider.
A program may use at most 1 GiB of HBM per device.

```python
import jax
import jax.numpy as jnp
from jax import lax

BATCH_SEQS = 8
CHUNK_LEN = 1024
CACHE_LEN = 2048
D_MODEL = 2560
NUM_HEADS = 32
HEAD_DIM = 80
FF_DIM = 4 * D_MODEL
LN_EPS = 1e-5


def setup_inputs(seed: int = 0, part: int = 0) -> dict:
    part_keys = jax.random.split(jax.random.fold_in(jax.random.key(seed), part), 5)
    shared_keys = jax.random.split(jax.random.key(seed + 7919), 12)
    max_start = CACHE_LEN - CHUNK_LEN
    starts = jax.random.randint(part_keys[1], (BATCH_SEQS,), 0, max_start + 1)
    longest = jax.random.randint(part_keys[2], (), 0, BATCH_SEQS)
    prefix_len = jnp.where(jnp.arange(BATCH_SEQS) == longest, max_start, starts).astype(jnp.int32)
    cache_shape = (BATCH_SEQS, CACHE_LEN, NUM_HEADS, HEAD_DIM)
    vec_shape = (D_MODEL,)
    d_scale = D_MODEL ** -0.5

    def normal_draw(key_in, shape_in, std_dev):
        return (std_dev * jax.random.normal(key_in, shape_in, jnp.float32)).astype(jnp.bfloat16)

    def gain_draw(key_in):
        return (1.0 + 0.25 * jax.random.normal(key_in, vec_shape, jnp.float32)).astype(jnp.bfloat16)

    return {
        'x_chunk': normal_draw(part_keys[0], (BATCH_SEQS, CHUNK_LEN, D_MODEL), 1.0),
        'prefix_len': prefix_len,
        'k_cache': normal_draw(part_keys[3], cache_shape, 1.0),
        'v_cache': normal_draw(part_keys[4], cache_shape, 1.0),
        'ln1_gain': gain_draw(shared_keys[0]),
        'ln1_bias': normal_draw(shared_keys[1], vec_shape, 0.25),
        'w_qkv': normal_draw(shared_keys[2], (D_MODEL, 3 * D_MODEL), d_scale),
        'b_qkv': normal_draw(shared_keys[3], (3 * D_MODEL,), 0.25),
        'w_out': normal_draw(shared_keys[4], (D_MODEL, D_MODEL), d_scale),
        'b_out': normal_draw(shared_keys[5], vec_shape, 0.25),
        'ln2_gain': gain_draw(shared_keys[6]),
        'ln2_bias': normal_draw(shared_keys[7], vec_shape, 0.25),
        'w_up': normal_draw(shared_keys[8], (D_MODEL, FF_DIM), d_scale),
        'b_up': normal_draw(shared_keys[9], (FF_DIM,), 0.25),
        'w_down': normal_draw(shared_keys[10], (FF_DIM, D_MODEL), FF_DIM ** -0.5),
        'b_down': normal_draw(shared_keys[11], vec_shape, 0.25),
    }


def layer_norm(tok_rows, ln_gain, ln_bias):
    rows_f32 = tok_rows.astype(jnp.float32)
    row_mean = jnp.mean(rows_f32, axis=-1, keepdims=True)
    centered = rows_f32 - row_mean
    row_var = jnp.mean(centered * centered, axis=-1, keepdims=True)
    normed = centered * lax.rsqrt(row_var + LN_EPS)
    return (normed * ln_gain.astype(jnp.float32) + ln_bias.astype(jnp.float32)).astype(jnp.bfloat16)


def write_rows(cache_seq, new_rows, start_pos):
    zero_idx = jnp.zeros_like(start_pos)
    return lax.dynamic_update_slice(cache_seq, new_rows, (start_pos, zero_idx, zero_idx))


def attend_one(operands):
    queries, keys_all, values_all, start_pos = operands
    scores = jnp.einsum('chd,thd->hct', queries.astype(jnp.float32), keys_all.astype(jnp.float32)) * (HEAD_DIM ** -0.5)
    slopes = jnp.exp2(-8.0 * (jnp.arange(NUM_HEADS) + 1).astype(jnp.float32) / NUM_HEADS)
    query_pos = start_pos + jnp.arange(CHUNK_LEN)
    rel_pos = (jnp.arange(CACHE_LEN)[None, :] - query_pos[:, None]).astype(jnp.float32)
    scores = scores + slopes[:, None, None] * rel_pos[None]
    scores = jnp.where((rel_pos <= 0.0)[None], scores, -1e30)
    attn_probs = jax.nn.softmax(scores, axis=-1).astype(jnp.bfloat16)
    context = jnp.einsum('hct,thd->chd', attn_probs.astype(jnp.float32), values_all.astype(jnp.float32))
    return context.astype(jnp.bfloat16).reshape(CHUNK_LEN, D_MODEL)


def reference(x_chunk, prefix_len, k_cache, v_cache, ln1_gain, ln1_bias, w_qkv, b_qkv, w_out, b_out, ln2_gain, ln2_bias, w_up, b_up, w_down, b_down):
    tok_rows = x_chunk.reshape(BATCH_SEQS * CHUNK_LEN, D_MODEL)
    normed = layer_norm(tok_rows, ln1_gain, ln1_bias)
    qkv_proj = jnp.dot(normed, w_qkv, preferred_element_type=jnp.float32) + b_qkv.astype(jnp.float32)
    qkv_heads = qkv_proj.astype(jnp.bfloat16).reshape(BATCH_SEQS, CHUNK_LEN, NUM_HEADS, 3, HEAD_DIM)
    k_upd = jax.vmap(write_rows)(k_cache, qkv_heads[:, :, :, 1], prefix_len)
    v_upd = jax.vmap(write_rows)(v_cache, qkv_heads[:, :, :, 2], prefix_len)
    context = lax.map(attend_one, (qkv_heads[:, :, :, 0], k_upd, v_upd, prefix_len))
    context = context.reshape(BATCH_SEQS * CHUNK_LEN, D_MODEL)
    attn_out = jnp.dot(context, w_out, preferred_element_type=jnp.float32)
    residual = (tok_rows.astype(jnp.float32) + attn_out + b_out.astype(jnp.float32)).astype(jnp.bfloat16)
    normed2 = layer_norm(residual, ln2_gain, ln2_bias)
    up_pre = jnp.dot(normed2, w_up, preferred_element_type=jnp.float32) + b_up.astype(jnp.float32)
    up_act = jax.nn.gelu(up_pre, approximate=True).astype(jnp.bfloat16)
    down_out = jnp.dot(up_act, w_down, preferred_element_type=jnp.float32)
    x_out = (residual.astype(jnp.float32) + down_out + b_down.astype(jnp.float32)).astype(jnp.bfloat16)
    return x_out.reshape(BATCH_SEQS, CHUNK_LEN, D_MODEL), k_upd, v_upd
```

```python
import functools
import jax
import jax.numpy as jnp
from jax import lax
from jax.sharding import PartitionSpec as P
from jax.experimental import pallas as pl
from jax.experimental.pallas import tpu as pltpu

LN_EPS = 1e-5
LOG2E = 1.4426950408889634
NEG = -1e30
KV_BLK = 256
Q_BLK = 512
CHUNKS = ((0, 3), (3, 3), (6, 2))


def ln_rows(rows_f32, gain, bias):
    row_mean = jnp.mean(rows_f32, axis=-1, keepdims=True)
    centered = rows_f32 - row_mean
    row_var = jnp.mean(centered * centered, axis=-1, keepdims=True)
    normed = centered * lax.rsqrt(row_var + LN_EPS)
    return (normed * gain.astype(jnp.float32) + bias.astype(jnp.float32)).astype(jnp.bfloat16)


def ln_body(x_ref, g_ref, b_ref, o_ref):
    o_ref[0] = ln_rows(x_ref[0].astype(jnp.float32), g_ref[...], b_ref[...])


def ln1_call(x_local, gain, bias, first, count):
    _, tok, feat = x_local.shape
    return pl.pallas_call(
        ln_body,
        grid=(count,),
        in_specs=[
            pl.BlockSpec((1, tok, feat), lambda i: (first + i, 0, 0)),
            pl.BlockSpec((1, feat), lambda i: (0, 0)),
            pl.BlockSpec((1, feat), lambda i: (0, 0)),
        ],
        out_specs=pl.BlockSpec((1, tok, feat), lambda i: (i, 0, 0)),
        out_shape=jax.ShapeDtypeStruct((count, tok, feat), jnp.bfloat16),
        name="ln1",
    )(x_local, gain.reshape(1, feat), bias.reshape(1, feat))


def attn_body(first, heads, dim, chunk, len_ref, slope_ref, x_ref, w_ref, bias_ref, kc_ref, vc_ref, *refs):
    o_ref, ko_ref, vo_ref, qkv_s, m_s, l_s, acc_s, ctx_s = refs[-8:]
    prefix = len_ref[first + pl.program_id(0)]
    feat = x_ref.shape[3]
    rows = x_ref[:, 0].reshape(chunk, feat)
    qkv_t = lax.dot_general(w_ref[...], rows, (((1,), (1,)), ((), ())), preferred_element_type=jnp.float32)
    qkv_t = (qkv_t + bias_ref[...].astype(jnp.float32)).astype(jnp.bfloat16)
    qkv_s[...] = qkv_t.reshape(heads * 3, dim, chunk)
    scale = (dim ** -0.5) * LOG2E
    kv_row = lax.broadcasted_iota(jnp.int32, (KV_BLK, 128), 0)
    lane = lax.broadcasted_iota(jnp.int32, (dim, 128), 1)
    base = (prefix // 128) * 128
    shift = prefix - base

    def write_cache(h, which, c_ref, out_ref):
        out_ref[0, h] = c_ref[0, h]
        fresh = qkv_s.at[3 * h + which]
        prev = None
        for i in range(chunk // 128 + 1):
            window = pl.ds(pl.multiple_of(base + 128 * i, 128), 128)
            if i < chunk // 128:
                cur = pltpu.roll(fresh[:, 128 * i:128 * (i + 1)].astype(jnp.float32), shift, 1)
                old = c_ref[0, h, :, window].astype(jnp.float32) if prev is None else prev
                out_ref[0, h, :, window] = jnp.where(lane < shift, old, cur).astype(jnp.bfloat16)
                prev = cur
            else:
                @pl.when(shift > 0)
                def _():
                    old = c_ref[0, h, :, window].astype(jnp.float32)
                    out_ref[0, h, :, window] = jnp.where(lane < shift, prev, old).astype(jnp.bfloat16)

    def update(h, lo, hi, k_blk, v_blk, bias, mask):
        s = lax.dot_general(k_blk, qkv_s[3 * h, :, lo:hi], (((0,), (0,)), ((), ())), preferred_element_type=jnp.float32)
        s = s * scale + jnp.concatenate([bias] * ((hi - lo) // 128), axis=1)
        if mask is not None:
            s = jnp.where(mask, s, NEG)
        m_prev = m_s[:, lo:hi]
        m_new = jnp.maximum(m_prev, jnp.max(s, axis=0, keepdims=True))
        alpha = jnp.exp2(m_prev - m_new)
        p = jnp.exp2(s - m_new)
        l_s[:, lo:hi] = l_s[:, lo:hi] * alpha + jnp.sum(p, axis=0, keepdims=True)
        m_s[:, lo:hi] = m_new
        pv = jnp.dot(v_blk, p.astype(jnp.bfloat16), preferred_element_type=jnp.float32)
        acc_s[:, lo:hi] = acc_s[:, lo:hi] * alpha + pv

    def one_head(h, carry):
        slope2 = slope_ref[0, h] * LOG2E
        m_s[...] = jnp.full_like(m_s, NEG)
        l_s[...] = jnp.zeros_like(l_s)
        acc_s[...] = jnp.zeros_like(acc_s)

        def cached(i, c):
            start = pl.multiple_of(i * KV_BLK, KV_BLK)
            k_blk = kc_ref[0, h, :, pl.ds(start, KV_BLK)]
            v_blk = vc_ref[0, h, :, pl.ds(start, KV_BLK)]
            pos = start - prefix + kv_row
            bias = jnp.where(pos < 0, slope2 * pos.astype(jnp.float32), NEG)
            for lo in range(0, chunk, Q_BLK):
                update(h, lo, lo + Q_BLK, k_blk, v_blk, bias, None)
            return c

        lax.fori_loop(0, (prefix + KV_BLK - 1) // KV_BLK, cached, 0)

        for j in range(0, chunk, KV_BLK):
            k_blk = qkv_s[3 * h + 1, :, j:j + KV_BLK]
            v_blk = qkv_s[3 * h + 2, :, j:j + KV_BLK]
            bias = slope2 * (j + kv_row).astype(jnp.float32)
            k_idx = lax.broadcasted_iota(jnp.int32, (KV_BLK, KV_BLK), 0)
            q_idx = lax.broadcasted_iota(jnp.int32, (KV_BLK, KV_BLK), 1)
            update(h, j, j + KV_BLK, k_blk, v_blk, bias, k_idx <= q_idx)
            if j + KV_BLK < chunk:
                update(h, j + KV_BLK, chunk, k_blk, v_blk, bias, None)
        ctx_s[h] = (acc_s[...] / l_s[...]).astype(jnp.bfloat16)
        write_cache(h, 1, kc_ref, ko_ref)
        write_cache(h, 2, vc_ref, vo_ref)
        return carry

    lax.fori_loop(0, heads, one_head, 0)
    tok = o_ref.shape[3]
    for p in range(chunk // tok):
        o_ref[p, 0] = ctx_s[:, :, p * tok:(p + 1) * tok].reshape(heads * dim, tok)


def attn_call(prefix_len, slopes, x_all, w_t, b_col, k_t, v_t, outs, first):
    parts, count, tok, feat = x_all.shape
    _, heads, dim, cache_len = k_t.shape
    chunk = parts * tok
    width = w_t.shape[0]
    cache_spec = pl.BlockSpec((1, heads, dim, cache_len), lambda b, n: (first + b, 0, 0, 0))
    in_specs = [
        pl.BlockSpec(memory_space=pltpu.SMEM),
        pl.BlockSpec((parts, 1, tok, feat), lambda b, n: (0, b, 0, 0)),
        pl.BlockSpec((width, feat), lambda b, n: (0, 0), pipeline_mode=pl.Buffered(1)),
        pl.BlockSpec((width, 1), lambda b, n: (0, 0), pipeline_mode=pl.Buffered(1)),
        cache_spec,
        cache_spec,
    ]
    ops = [prefix_len, slopes, x_all, w_t, b_col, k_t, v_t]
    aliases = {}
    if outs is not None:
        in_specs += [pl.BlockSpec(memory_space=pl.ANY)] * 2
        aliases = {len(ops): 1, len(ops) + 1: 2}
        ops += list(outs)
    grid_spec = pltpu.PrefetchScalarGridSpec(
        num_scalar_prefetch=1,
        grid=(count,),
        in_specs=in_specs,
        out_specs=(pl.BlockSpec((parts, 1, heads * dim, tok), lambda b, n: (0, b, 0, 0)), cache_spec, cache_spec),
        scratch_shapes=[
            pltpu.VMEM((heads * 3, dim, chunk), jnp.bfloat16),
            pltpu.VMEM((1, chunk), jnp.float32),
            pltpu.VMEM((1, chunk), jnp.float32),
            pltpu.VMEM((dim, chunk), jnp.float32),
            pltpu.VMEM((heads, dim, chunk), jnp.bfloat16),
        ],
    )
    return pl.pallas_call(
        functools.partial(attn_body, first, heads, dim, chunk),
        grid_spec=grid_spec,
        out_shape=(
            jax.ShapeDtypeStruct((parts, count, heads * dim, tok), jnp.bfloat16),
            jax.ShapeDtypeStruct(k_t.shape, k_t.dtype),
            jax.ShapeDtypeStruct(v_t.shape, v_t.dtype),
        ),
        input_output_aliases=aliases,
        name="attend",
    )(*ops)


def out_body(per, w_ref, ctx_ref, x_ref, bo_ref, g_ref, b_ref, r_ref, a_ref, acc_s):
    step = pl.program_id(0)
    parts, _, width, tok = ctx_ref.shape
    half = w_ref.shape[2]
    ctx = jnp.concatenate([ctx_ref[:, b].reshape(parts * width, tok) for b in range(per)], axis=1)
    for i in range(2):
        cols = slice(i * half, (i + 1) * half)
        val = lax.dot_general(ctx, w_ref[i], (((0,), (0,)), ((), ())), preferred_element_type=jnp.float32)

        @pl.when(step == 0)
        def _():
            acc_s[:, cols] = val

        @pl.when(step > 0)
        def _():
            acc_s[:, cols] += val

    @pl.when(step == pl.num_programs(0) - 1)
    def _():
        def block(i, c):
            rows = pl.ds(pl.multiple_of(i * 64, 64), 64)
            r = (x_ref[rows, :].astype(jnp.float32) + acc_s[rows, :] + bo_ref[...].astype(jnp.float32)).astype(jnp.bfloat16)
            r_ref[rows, :] = r
            a_ref[rows, :] = ln_rows(r.astype(jnp.float32), g_ref[...], b_ref[...])
            return c

        lax.fori_loop(0, x_ref.shape[0] // 64, block, 0)


def out_call(ctx, w_full, x_rows, b_out, gain, bias, first):
    parts, per, width, tok = ctx.shape
    feat = x_rows.shape[1]
    rows = per * tok
    blk = 4
    vec = pl.BlockSpec((1, feat), lambda i: (0, 0))
    row = pl.BlockSpec((rows, feat), lambda i: (0, 0))
    return pl.pallas_call(
        functools.partial(out_body, per),
        grid=(parts // blk,),
        in_specs=[
            pl.BlockSpec((2, blk * width, feat // 2), lambda i: (0, i, 0)),
            pl.BlockSpec((blk, per, width, tok), lambda i: (i, 0, 0, 0)),
            pl.BlockSpec((rows, feat), lambda i: (first // per, 0)),
            vec, vec, vec,
        ],
        out_specs=(row, row),
        out_shape=(jax.ShapeDtypeStruct((rows, feat), jnp.bfloat16),) * 2,
        scratch_shapes=[pltpu.VMEM((rows, feat), jnp.float32)],
        name="out_proj",
    )(w_full, ctx, x_rows, b_out.reshape(1, feat), gain.reshape(1, feat), bias.reshape(1, feat))


def finish_body(acc_ref, part_ref, r_ref, bd_ref, *refs):
    o_ref = refs[-1]
    total = r_ref[...].astype(jnp.float32) + (acc_ref[...] + part_ref[...].astype(jnp.float32))
    o_ref[...] = (total + bd_ref[...].astype(jnp.float32)).astype(jnp.bfloat16)


def finish_call(acc, part, resid, b_down, out, rows_all, first):
    rows, feat = resid.shape
    blk = 128
    row = pl.BlockSpec((blk, feat), lambda i: (i, 0))
    ops = [acc, part, resid, b_down.reshape(1, feat)]
    specs = [row, row, row, pl.BlockSpec((1, feat), lambda i: (0, 0))]
    aliases = {}
    if out is not None:
        aliases = {len(ops): 0}
        ops.append(out)
        specs.append(pl.BlockSpec(memory_space=pl.ANY))
    return pl.pallas_call(
        finish_body,
        grid=(rows // blk,),
        in_specs=specs,
        out_specs=pl.BlockSpec((blk, feat), lambda i: (first // blk + i, 0)),
        out_shape=jax.ShapeDtypeStruct((rows_all, feat), jnp.bfloat16),
        input_output_aliases=aliases,
        name="finish",
    )(*ops)


def mlp_body(near, count, has_acc, n_parts, n_last, tiles, z_ref, *refs):
    parts, refs = refs[:n_parts], refs[n_parts:]
    shards = [refs[7 * n:7 * n + 7] for n in range(count)]
    rest = list(refs[7 * count:])
    acc_in = rest.pop(0) if has_acc else None
    last, rest = rest[:n_last], rest[n_last:]
    out_ref, h_s = rest[:2]
    a_s = parts[0] if n_parts == 1 else rest[2]
    step = pl.program_id(0)
    rows, feat = parts[0].shape
    half = feat // 2
    width = shards[0][0].shape[1]
    order = [0 if n < near else z_ref[0] for n in range(count)]

    if n_parts > 1:
        @pl.when(step == 0)
        def _():
            for i, part_ref in enumerate(parts):
                a_s[i * rows:(i + 1) * rows] = part_ref[...]

    @pl.when(step < tiles)
    def _():
        cols = pl.ds(pl.multiple_of(step * width, width), width)
        for n, (ua_ref, ub_ref, bias_ref, *_) in enumerate(shards):
            lo = pl.ds(pl.multiple_of(order[n] * half, half), half)
            hi = pl.ds(pl.multiple_of((1 - order[n]) * half, half), half)
            pre = jnp.dot(a_s[:, lo], ua_ref[...], preferred_element_type=jnp.float32)
            pre = pre + jnp.dot(a_s[:, hi], ub_ref[...], preferred_element_type=jnp.float32)
            pre = pre + bias_ref[...].astype(jnp.float32)
            h_s[n, :, cols] = jax.nn.gelu(pre, approximate=True).astype(jnp.bfloat16)

    @pl.when(step >= tiles)
    def _():
        for side in range(2):
            start = (step - tiles) * width + side * half
            cols = pl.ds(pl.multiple_of(start, width), width)
            val = acc_in[:, cols] if has_acc else None
            for n, refs_n in enumerate(shards):
                if n < near:
                    down = jnp.concatenate([refs_n[3 + 2 * side][...], refs_n[4 + 2 * side][...]], axis=0)
                else:
                    down = jnp.where(
                        order[n] == side,
                        jnp.concatenate([refs_n[3][...], refs_n[4][...]], axis=0),
                        jnp.concatenate([refs_n[5][...], refs_n[6][...]], axis=0))
                part = jnp.dot(h_s[n], down, preferred_element_type=jnp.float32)
                val = part if val is None else val + part
            if n_last:
                r_ref, part_ref, bd_ref = last[:3]
                val = r_ref[:, cols].astype(jnp.float32) + (val + part_ref[:, cols].astype(jnp.float32))
                val = val + bd_ref[:, cols].astype(jnp.float32)
            out_ref[:, cols] = val.astype(out_ref.dtype)


def mlp_call(z_arr, parts, near, far, acc, acc_part, out_type, last=(), place=(0, 1)):
    rows, feat = parts[0].shape
    total = rows * len(parts)
    half = feat // 2
    width = 256
    tiles = half // width
    one = pl.Buffered(1)
    full = lambda r: pl.BlockSpec((r, feat), lambda i, z: (0, 0), pipeline_mode=one)
    specs = [full(rows)] * len(parts)
    ops = [z_arr, *parts]
    up_t = lambda i: jnp.minimum(i, tiles - 1)
    down_t = lambda i: jnp.maximum(i - tiles, 0)
    for n, (up_a, up_b, bias_row, *downs) in enumerate([*near, *far]):
        hid = bias_row.shape[1]
        assert hid == half
        is_far = n >= len(near)
        places = ((0, 0), (0, 0), (0, 0), (0, 0)) if is_far else ((0, 0), (1, 0), (0, tiles), (1, tiles))
        specs += [
            pl.BlockSpec((half, width), lambda i, z: (0, up_t(i))),
            pl.BlockSpec((half, width), lambda i, z, o=0 if is_far else 1: (o, up_t(i))),
            pl.BlockSpec((1, width), lambda i, z: (0, up_t(i))),
            *[pl.BlockSpec((hid // 2, width), lambda i, z, r=r, o=o: (r, o + down_t(i))) for r, o in places],
        ]
        ops += [up_a, up_b, bias_row, *downs]
    count = len(near) + len(far)
    scratch = [pltpu.VMEM((count, total, half), jnp.bfloat16)]
    if len(parts) > 1:
        scratch.append(pltpu.VMEM((total, feat), jnp.bfloat16))
    if acc is not None:
        specs.append(pl.BlockSpec((rows, feat), lambda i, z: (acc_part, 0), pipeline_mode=one))
        ops.append(acc)
    aliases = {}
    if last:
        specs += [full(rows), full(rows), full(1)]
        ops += [last[0], last[1], last[2].reshape(1, feat)]
        if len(last) > 3:
            aliases = {len(ops): 0}
            specs.append(pl.BlockSpec(memory_space=pl.ANY))
            ops.append(last[3])
    index, blocks = place
    return pl.pallas_call(
        functools.partial(mlp_body, len(near), count, acc is not None, len(parts), len(last), tiles),
        grid_spec=pltpu.PrefetchScalarGridSpec(
            num_scalar_prefetch=1,
            grid=(2 * tiles,),
            in_specs=specs,
            out_specs=pl.BlockSpec((total, feat), lambda i, z: (index, 0), pipeline_mode=one),
            scratch_shapes=scratch,
        ),
        out_shape=jax.ShapeDtypeStruct((blocks, feat) if last else (total, feat), out_type),
        input_output_aliases=aliases,
        name="mlp",
    )(*ops)


def solution(mesh):
    tp_size = mesh.shape['tp']
    dp_size = mesh.shape['dp']

    def local_layer(x_local, prefix_len, k_cache, v_cache, ln1_gain, ln1_bias, w_qkv, b_qkv, w_out, b_out, ln2_gain, ln2_bias, w_up, b_up, w_down, b_down):
        batch_n, tok, feat = x_local.shape
        heads = k_cache.shape[2]
        group = lax.axis_index('dp')
        head_ids = lax.axis_index('tp') * heads + jnp.arange(heads)
        slopes = jnp.exp2(-8.0 * (head_ids + 1).astype(jnp.float32) / (heads * tp_size)).reshape(1, heads)

        z_arr = group.reshape(1)
        half = feat // 2
        core_x = [(i, i ^ 1) for i in range(tp_size)]
        chip_x = [(i, i ^ 2) for i in range(tp_size)]
        chip_y = [(i, i ^ 4) for i in range(tp_size)]

        def over(v, pairs):
            return lax.ppermute(v, 'tp', pairs)

        def over_z(v):
            return lax.ppermute(v, 'dp', [(0, 1), (1, 0)])

        normed = [ln1_call(x_local, ln1_gain, ln1_bias, first, count) for first, count in CHUNKS]
        bias_all = lax.all_gather(b_up.reshape(1, -1), 'tp', axis=0, tiled=True)
        me = lax.axis_index('tp')
        bias_of = lambda k: lax.dynamic_slice_in_dim(bias_all, me ^ k, 1, axis=0)

        up_mine = lax.dynamic_slice_in_dim(w_up, group * half, half, axis=0)
        down_mine = lax.dynamic_slice_in_dim(w_down, group * half, half, axis=1)
        hid_half = down_mine.shape[0] // 2
        up_y = over(up_mine, chip_y)
        down_y = [over(down_mine[:hid_half], chip_y), over(down_mine[hid_half:], chip_y)]
        up_c, down_c = over(w_up, core_x), over(w_down, core_x)
        up_yz, up_yc = over_z(up_y), over(up_y, core_x)
        up_yzc = over(up_yz, core_x)
        down_yz = [over_z(v) for v in down_y]
        down_yc = [over(v, core_x) for v in down_y]
        down_yzc = [over(v, core_x) for v in down_yz]

        gathered = []
        for rows in normed:
            gathered.append(lax.all_gather(rows, 'tp', axis=0, tiled=False))
        out_mine = lax.dynamic_slice_in_dim(w_out, group * half, half, axis=1)
        w_out_full = lax.all_gather(out_mine, ('dp', 'tp'), axis=0, tiled=False).reshape(dp_size, feat, half)

        k_t = jnp.transpose(k_cache, (0, 2, 3, 1))
        v_t = jnp.transpose(v_cache, (0, 2, 3, 1))
        w_t = jnp.transpose(w_qkv)
        b_col = b_qkv.reshape(-1, 1)
        x_rows = x_local.reshape(batch_n * tok, feat)
        near = [(w_up, w_up, bias_of(0), *[w_down] * 4), (up_c, up_c, bias_of(1), *[down_c] * 4)]
        far = [(up_y, up_yz, bias_of(4), *down_y, *down_yz), (up_yc, up_yzc, bias_of(5), *down_yc, *down_yzc)]
        outs, done = None, []
        for i, (first, _) in enumerate(CHUNKS):
            ctx, *outs = attn_call(prefix_len, slopes, gathered[i], w_t, b_col, k_t, v_t, outs, first)
            ctx = lax.all_to_all(ctx, 'tp', split_axis=0, concat_axis=0, tiled=True)
            resid, normed2 = out_call(ctx, w_out_full, x_rows, b_out, ln2_gain, ln2_bias, first)
            other2 = over(normed2, chip_x)
            acc = mlp_call(z_arr, [normed2, other2] if i < 2 else [normed2], near, [], None, 0, jnp.float32)
            if i < 2:
                send = mlp_call(z_arr, [other2], [], far, acc, 1, jnp.bfloat16)
            else:
                send = mlp_call(z_arr, [other2], near, far, None, 0, jnp.bfloat16)
            done.append((normed2, acc, over(send, chip_x), resid, first * tok))
        x_out, rows_all = None, batch_n * tok
        for i, (normed2, acc, part, resid, start) in enumerate(done):
            if i < 2:
                last = (resid, part, b_down) + (() if x_out is None else (x_out,))
                x_out = mlp_call(z_arr, [normed2], [], far, acc, 0, jnp.bfloat16, last, (start // resid.shape[0], rows_all))
            else:
                keep = mlp_call(z_arr, [normed2], [], far, acc, 0, jnp.float32)
            if i == 2:
                x_out = finish_call(keep, part, resid, b_down, x_out, rows_all, start)
        k_upd, v_upd = [jnp.transpose(o, (0, 3, 1, 2)) for o in outs]
        return x_out.reshape(batch_n, tok, feat), k_upd, v_upd

    tok_spec = P('dp', 'tp', None)
    cache_spec = P('dp', None, 'tp', None)
    replicated = P()
    in_specs = (tok_spec, P('dp'), cache_spec, cache_spec, replicated, replicated, P(None, 'tp'), P('tp'), P('tp', None), replicated, replicated, replicated, P(None, 'tp'), P('tp'), P('tp', None), replicated)
    return jax.shard_map(local_layer, mesh=mesh, in_specs=in_specs, out_specs=(tok_spec, cache_spec, cache_spec), check_vma=False)
```
